32 devices in a mesh: dp: 4 (over y, x), owner: 8 (over z, core).
Axes of the slice: x: 2, y: 2, z: 4, core: 2. Of those that a mesh axis runs over, the one named last changes fastest.
Arguments:
- partial_grads: bfloat16 [4, 48, 1024, 1024], P('dp', None, 'owner'), may hold values from -2.09375 to 2.09375
- owner_map: int32 [48], replicated, may hold values from 0 to 7, as said below
- left_stats: float32 [8, 12, 1024, 1024], P('owner', None, 'dp'), may hold values from -1.8 to 1.8
- right_stats: float32 [8, 12, 1024, 1024], P('owner', None, 'dp'), may hold values from -1.8 to 1.8
- left_roots: bfloat16 [8, 12, 1024, 1024], P('owner', None, 'dp'), as said below
- right_roots: bfloat16 [8, 12, 1024, 1024], P('owner', None, 'dp'), as said below
Outputs:
- direction: bfloat16 [48, 1024, 1024], P(None, ('dp', 'owner'))
- new_left_stats: float32 [8, 12, 1024, 1024], P('owner', None, 'dp')
- new_right_stats: float32 [8, 12, 1024, 1024], P('owner', None, 'dp')
The draws below stay inside these ranges and needn't reach their ends.
Inputs may be any that keep to these rules, and one draw needn't show every extreme that they name: `owner_map`: no owner index holds more than 12 blocks, and some owner holds exactly 12. `left_roots`: each block is dense and not symmetric; its diagonal entries are of order one and its off-diagonal entries are small. `right_roots`: each block is dense and not symmetric; its diagonal entries are of order one and its off-diagonal entries are small.
All inputs are finite; a program needn't handle non-finite values.
Results may differ from the reference program's by a relative error of at most 0.017.
Values may be sent and summed in bfloat16 or wider, within the bound.
No kernel may reach another device: no remote copies, remote signals or barrier semaphores. Data moves between devices by JAX's collectives and lax.ppermute only.
A program may use at most 256 MiB of HBM per device.

```python
import jax
import jax.numpy as jnp
from jax import lax

D_MODEL = 2560
D_IN = 10576
D_INNER = 5120
TILE = 1024
TILES = 48
OWNERS = 8
SLOTS = 12
N_DP = 4


def draw_owner_map(key, part):
    first, second = jax.random.split(jax.random.fold_in(key, 7))
    total = OWNERS * SLOTS
    ranks = jax.random.permutation(first, total).astype(jnp.int32)
    chosen = jax.random.randint(second, (), 0, OWNERS, dtype=jnp.int32)
    ids = jnp.arange(total, dtype=jnp.int32)
    keyed = jnp.where(ids // SLOTS == chosen, -1 - ids % SLOTS, ranks)
    order = jnp.argsort(keyed, stable=True).astype(jnp.int32)
    return (order[:TILES] // SLOTS).astype(jnp.int32)


def draw_root(key):
    first, second = jax.random.split(key)
    shape = (OWNERS, SLOTS, TILE, TILE)
    diag = jax.random.uniform(first, (OWNERS, SLOTS, TILE), jnp.float32, 0.5, 1.5)
    off = jax.random.normal(second, shape, jnp.float32) * (0.4 / TILE ** 0.5)
    eye = jnp.eye(TILE, dtype=jnp.float32)
    return off + diag[..., None] * eye


def draw_left_roots(key, part):
    return draw_root(jax.random.fold_in(key, 11)).astype(jnp.bfloat16)


def draw_right_roots(key, part):
    return draw_root(jax.random.fold_in(key, 13)).astype(jnp.bfloat16)


def shard_levels(own_key, shape, shards, least, high):
    level = 1.0
    for position, shards_of in shards:
        draws = jax.random.uniform(jax.random.fold_in(jax.random.fold_in(own_key, 6), position), (shards_of,), jnp.float32, least / len(shards), high / len(shards))
        level = level * jnp.repeat(jnp.exp(draws), shape[position] // shards_of).reshape((-1,) + (1,) * (len(shape) - 1 - position))
    return level


def centred(key, shape, deviation, limit, shards=(), kind=jnp.bfloat16):
    values = deviation * jax.random.normal(key, shape, jnp.float32)
    if shards:
        values = values * shard_levels(key, shape, shards, -0.22, 0.18)
    return jnp.clip(values, -limit, limit).astype(kind)


def setup_inputs(seed: int = 0) -> dict:
    key_of = jax.random.split(jax.random.key(seed), 7)
    partial_grads = centred(key_of[0], (N_DP, TILES, TILE, TILE), 0.35, 2.09375, ((0, 4), (2, 8)))
    owner_map = draw_owner_map(jax.random.fold_in(key_of[6], 71), 0)
    left_stats = centred(key_of[2], (OWNERS, SLOTS, TILE, TILE), 0.3, 1.8, ((0, 8), (2, 4)), jnp.float32)
    right_stats = centred(key_of[3], (OWNERS, SLOTS, TILE, TILE), 0.3, 1.8, ((0, 8), (2, 4)), jnp.float32)
    left_roots = draw_left_roots(jax.random.fold_in(key_of[6], 71), 0)
    right_roots = draw_right_roots(jax.random.fold_in(key_of[6], 71), 0)
    return {"partial_grads": partial_grads, "owner_map": owner_map, "left_stats": left_stats, "right_stats": right_stats, "left_roots": left_roots, "right_roots": right_roots}


stat_decay = 0.999


def extents(count):
    index = jnp.arange(count, dtype=jnp.int32)
    in_cols = -(-D_IN // TILE)
    out_cols = -(-D_MODEL // TILE)
    in_count = (-(-D_MODEL // TILE)) * in_cols
    is_in = index < in_count
    other = jnp.maximum(index - in_count, 0)
    rows = jnp.where(is_in, jnp.minimum(TILE, D_MODEL - (index // in_cols) * TILE), jnp.minimum(TILE, D_INNER - (other // out_cols) * TILE))
    cols = jnp.where(is_in, jnp.minimum(TILE, D_IN - (index % in_cols) * TILE), jnp.minimum(TILE, D_MODEL - (other % out_cols) * TILE))
    return rows.astype(jnp.int32), cols.astype(jnp.int32)


def reference(partial_grads, owner_map, left_stats, right_stats, left_roots, right_roots):
    rows, cols = extents(TILES)
    line = jnp.arange(TILE, dtype=jnp.int32)
    mask = (line[None, :, None] < rows[:, None, None]) & (line[None, None, :] < cols[:, None, None])
    total = jnp.zeros(partial_grads.shape[1:], jnp.float32)
    for source in range(N_DP):
        total = total + partial_grads[source].astype(jnp.float32)
    grads = jnp.where(mask, total, jnp.float32(0.0)).astype(jnp.bfloat16)
    ids = jnp.arange(TILES, dtype=jnp.int32)
    same = (owner_map[:, None] == owner_map[None, :]) & (ids[None, :] < ids[:, None])
    slot = jnp.sum(same.astype(jnp.int32), axis=1).astype(jnp.int32)

    def per_tile(index):
        grad = grads[index]
        owner = owner_map[index]
        place = slot[index]
        left_new = stat_decay * left_stats[owner, place] + (1.0 - stat_decay) * jnp.dot(grad, grad.T, preferred_element_type=jnp.float32)
        right_new = stat_decay * right_stats[owner, place] + (1.0 - stat_decay) * jnp.dot(grad.T, grad, preferred_element_type=jnp.float32)
        left_part = jnp.dot(left_roots[owner, place], grad, preferred_element_type=jnp.float32).astype(jnp.bfloat16)
        result = jnp.dot(left_part, right_roots[owner, place], preferred_element_type=jnp.float32)
        result = jnp.where(mask[index], result, jnp.float32(0.0)).astype(jnp.bfloat16)
        return left_new, right_new, result

    left_all, right_all, direction = lax.map(per_tile, ids)
    new_left = (stat_decay * left_stats).at[owner_map, slot].set(left_all)
    new_right = (stat_decay * right_stats).at[owner_map, slot].set(right_all)
    return (direction, new_left, new_right)
```

```python
import jax
import jax.numpy as jnp
from jax import lax
from jax.experimental import pallas as pl
from jax.experimental.pallas import tpu as pltpu
from jax.sharding import PartitionSpec as P


D_MODEL = 2560
D_IN = 10576
D_INNER = 5120
TILE = 1024
CHUNKS = 3


stat_decay = 0.999


def extents(count):
    index = jnp.arange(count, dtype=jnp.int32)
    in_cols = -(-D_IN // TILE)
    out_cols = -(-D_MODEL // TILE)
    in_count = -(-D_MODEL // TILE) * in_cols
    is_in = index < in_count
    other = jnp.maximum(index - in_count, 0)
    rows = jnp.where(
        is_in,
        jnp.minimum(TILE, D_MODEL - index // in_cols * TILE),
        jnp.minimum(TILE, D_INNER - other // out_cols * TILE),
    )
    cols = jnp.where(
        is_in,
        jnp.minimum(TILE, D_IN - index % in_cols * TILE),
        jnp.minimum(TILE, D_MODEL - other % out_cols * TILE),
    )
    return (rows, cols)


def bounds(slots):
    chunks = min(CHUNKS, slots)
    edges = [slots * i // chunks for i in range(chunks + 1)]
    return list(zip(edges[:-1], edges[1:]))


def step_kernel(meta, g_ref, r_ref, l_ref, ls_ref, rs_ref, *rest):
    res_ref, nl_ref, nr_ref, grad = rest[-4:]
    step = pl.program_id(0)
    groups, sources, _, q, tile = g_ref.shape
    lanes = l_ref.shape[1]
    for o in range(sources):
        for d in range(groups):
            grad[pl.ds((o * groups + d) * q, q), :] = g_ref[d, o, 0]
    base = pl.multiple_of(meta[0] * lanes, lanes)
    whole = grad[...]
    left = lax.dot_general(
        l_ref[0], whole, (((1,), (0,)), ((), ())), preferred_element_type=jnp.float32
    ).astype(jnp.bfloat16)
    product = lax.dot_general(
        left,
        r_ref[:, 0].reshape(tile, tile),
        (((1,), (0,)), ((), ())),
        preferred_element_type=jnp.float32,
    )
    row = base + lax.broadcasted_iota(jnp.int32, product.shape, 0)
    col = lax.broadcasted_iota(jnp.int32, product.shape, 1)
    keep = (row < meta[1 + 2 * step]) & (col < meta[2 + 2 * step])
    result = jnp.where(keep, product, 0.0).astype(jnp.bfloat16)
    res_ref[:, 0] = result.reshape(res_ref.shape[0], res_ref.shape[2], tile)
    gram = lax.dot_general(
        grad[pl.ds(base, lanes), :], whole, (((1,), (1,)), ((), ())), preferred_element_type=jnp.float32
    )
    nl_ref[0] = stat_decay * ls_ref[0] + (1.0 - stat_decay) * gram
    gram = lax.dot_general(
        grad[:, pl.ds(base, lanes)], whole, (((0,), (0,)), ((), ())), preferred_element_type=jnp.float32
    )
    nr_ref[0] = stat_decay * rs_ref[0] + (1.0 - stat_decay) * gram


def step_call(meta, grads, rights, lefts, left_stats, right_stats, prior, first, owners):
    groups, sources, count, q, tile = grads.shape
    _, lanes = lefts.shape[:2]
    sub = lanes // owners
    parts = owners if sub % 16 == 0 else 1
    slab = pl.BlockSpec((1, lanes, tile), lambda s, m: (first + s, 0, 0))
    specs = [
        pl.BlockSpec((groups, sources, 1, q, tile), lambda s, m: (0, 0, s, 0, 0)),
        pl.BlockSpec((rights.shape[0], 1, lanes, tile), lambda s, m: (0, first + s, 0, 0)),
        slab,
        slab,
        slab,
    ]
    operands = [grads, rights, lefts, left_stats, right_stats]
    aliases = {}
    if prior is not None:
        specs += [pl.BlockSpec(memory_space=pl.ANY)] * 2
        operands += list(prior)
        aliases = {6: 1, 7: 2}
    result, new_left, new_right = pl.pallas_call(
        step_kernel,
        grid_spec=pltpu.PrefetchScalarGridSpec(
            num_scalar_prefetch=1,
            grid=(count,),
            in_specs=specs,
            out_specs=[
                pl.BlockSpec((parts, 1, lanes // parts, tile), lambda s, m: (0, s, 0, 0)),
                slab,
                slab,
            ],
            scratch_shapes=[pltpu.VMEM((tile, tile), jnp.bfloat16)],
        ),
        out_shape=[
            jax.ShapeDtypeStruct((parts, count, lanes // parts, tile), jnp.bfloat16),
            jax.ShapeDtypeStruct(left_stats.shape, jnp.float32),
            jax.ShapeDtypeStruct(right_stats.shape, jnp.float32),
        ],
        input_output_aliases=aliases,
        cost_estimate=pl.CostEstimate(
            flops=8 * count * lanes * tile * tile,
            bytes_accessed=count * (4 * tile * tile + 20 * lanes * tile),
            transcendentals=0,
        ),
        compiler_params=pltpu.CompilerParams(vmem_limit_bytes=48 * 1024 * 1024),
    )(meta, *operands)
    if parts == 1:
        result = result[0].reshape(count, owners, sub, tile).transpose(1, 0, 2, 3)
    return result, new_left, new_right


def body(partial_grads, owner_map, left_stats, right_stats, left_roots, right_roots):
    owners = lax.axis_size("owner")
    owner_here = lax.axis_index("owner")
    dp_here = lax.axis_index("dp").astype(jnp.int32)
    tiles = owner_map.shape[0]
    slots = left_stats.shape[1]
    tile = left_stats.shape[3]
    piece = partial_grads.shape[2]
    rows, cols = extents(tiles)
    line = jnp.arange(tile, dtype=jnp.int32)
    ids = jnp.arange(tiles, dtype=jnp.int32)
    shares = lax.psum_scatter(partial_grads[0], "dp", scatter_dimension=1, tiled=True)
    q = shares.shape[1]
    same = (owner_map[:, None] == owner_map[None, :]) & (ids[None, :] < ids[:, None])
    slot = jnp.sum(same.astype(jnp.int32), axis=1)
    picks = (slot[None, None, :] == jnp.arange(slots, dtype=jnp.int32)[None, :, None]) & (
        owner_map[None, None, :] == jnp.arange(owners, dtype=jnp.int32)[:, None, None]
    )
    tile_of = jnp.sum(jnp.where(picks, ids, 0), axis=2)
    rows_of = jnp.sum(jnp.where(picks, rows, 0), axis=2)
    cols_of = jnp.sum(jnp.where(picks, cols, 0), axis=2)
    rows_here = lax.dynamic_index_in_dim(rows_of, owner_here, 0, keepdims=False)
    cols_here = lax.dynamic_index_in_dim(cols_of, owner_here, 0, keepdims=False)
    extent_here = jnp.stack([rows_here, cols_here], axis=1)
    share_rows = owner_here * piece + dp_here * q + jnp.arange(q, dtype=jnp.int32)
    shares, roots = lax.optimization_barrier((shares, right_roots[0]))
    rights = lax.all_gather(roots, "dp", axis=0)
    prior = None
    direction = None

    def place(direction, returned, number):
        first, last = bounds(slots)[number]
        count = last - first
        flat = returned.reshape((owners * count,) + returned.shape[2:])
        local = slot - first
        here = (local >= 0) & (local < count)
        spot = owner_map * count + jnp.clip(local, 0, count - 1)
        chosen = flat.at[spot].get(mode="promise_in_bounds")
        if direction is None:
            return chosen
        return jnp.where(here[:, None, None], chosen, direction)

    for number, (first, last) in enumerate(bounds(slots)):
        count = last - first
        taken = shares.at[tile_of[:, first:last].reshape(-1)].get(mode="promise_in_bounds")
        taken = taken.reshape((owners, count) + shares.shape[1:])
        inside = (share_rows[None, None, :, None] < rows_of[:, first:last, None, None]) & (
            line[None, None, None, :] < cols_of[:, first:last, None, None]
        )
        taken = jnp.where(inside, taken, jnp.zeros((), shares.dtype))
        arrived = lax.all_to_all(taken, "owner", split_axis=0, concat_axis=0, tiled=True)
        grads = lax.all_gather(arrived, "dp", axis=0)
        if q % 16:
            grads = grads.transpose(2, 1, 0, 3, 4).reshape(1, 1, count, tile, tile)
        if number:
            grads, returned = lax.optimization_barrier((grads, returned))
            direction = place(direction, returned, number - 1)
        meta = jnp.concatenate([dp_here[None], extent_here[first:last].reshape(-1)])
        result, *prior = step_call(
            meta, grads, rights, left_roots[0], left_stats[0], right_stats[0], prior, first, owners
        )
        returned = lax.all_to_all(result, "owner", split_axis=0, concat_axis=0, tiled=True)
    direction = place(direction, returned, number)
    new_left, new_right = prior
    return (direction, new_left[None], new_right[None])


def solution(mesh):
    placed = (
        P("dp", None, "owner", None),
        P(),
        P("owner", None, "dp", None),
        P("owner", None, "dp", None),
        P("owner", None, "dp", None),
        P("owner", None, "dp", None),
    )
    return jax.shard_map(
        body,
        mesh=mesh,
        in_specs=placed,
        out_specs=(
            P(None, ("dp", "owner"), None),
            P("owner", None, "dp", None),
            P("owner", None, "dp", None),
        ),
        check_vma=False,
    )
```
